32 devices in a mesh: groups: 2 (over x), blk: 16 (over z, y, core).
Axes of the slice: x: 2, y: 2, z: 4, core: 2. Of those that a mesh axis runs over, the one named last changes fastest.
Arguments:
- tokens: bfloat16 [2048, 4096], P(('groups', 'blk')), parts along dimension 0, may hold values from -9 to 9, as said below
- blocks: bfloat16 [16, 7, 128, 128], P('blk'), may hold values from -0.5 to 0.5
- counts: int32 [2, 8], replicated, may hold values from 1 to 7, 48 in all within a row
- block_rows: int32 [16, 7], replicated, may hold values from 0 to 31
- block_cols: int32 [16, 7], replicated, may hold values from 0 to 111
Outputs:
- up: bfloat16 [2048, 14336], P(('groups', 'blk')), parts along dimension 0
- col_rms: float32 [28672], P('groups'), parts along dimension 0
The draws below stay inside these ranges and needn't reach their ends.
There are 2 independent parts, one for each index of `groups`. The reference program is written for one: setup_inputs(seed, part) draws one part's arguments, and reference() takes and returns one part's arrays. A program takes and returns all parts, laid end to end along the dimension named above; an argument that names none is the same for every part. Nothing has to cross between parts.
Inputs may be any that keep to these rules, and one draw needn't show every extreme that they name: `tokens`: scale of a token's entries grows with its position in the sequence. `counts`: each row sums to 48, and each row has an entry equal to 7. `block_rows`: slots at or past an owner's count carry no block and are ignored, whatever they hold. `block_cols`: slots at or past an owner's count are ignored.
All inputs are finite; a program needn't handle non-finite values.
Results may differ from the reference program's by a relative error of at most 0.001.
Values may be sent and summed in bfloat16 or wider, within the bound.
A program may use at most 192 MiB of HBM per device.

```python
import math
import jax
import jax.numpy as jnp
import numpy as np
from jax import lax

D = 4096
FFW = 14336
BS = 128
MAXB = 7
AVG = 6
BAL = 8
OWNERS = 16
TOKENS = 1024
ROWB = 32
COLB = 112


def draw_tokens(key, part):
    position = jnp.arange(TOKENS, dtype=jnp.float32)[:, None] / TOKENS
    values = jnp.clip(jax.random.normal(key, (TOKENS, D), jnp.float32), -5.0, 5.0)
    scale = jnp.sqrt(1.0 + 2.0 * position)
    return (values * scale).astype(jnp.bfloat16)


def place_ends(array, stream_key, smallest, largest):
    longest = array.shape.index(max(array.shape))
    spots = []
    for shift in (0, 1):
        where = [jax.random.randint(jax.random.fold_in(stream_key, axis), (), 0, length) for axis, length in enumerate(array.shape)]
        where[longest] = (where[longest] + shift) % array.shape[longest]
        spots.append(tuple(where))
    return array.at[spots[0]].set(smallest).at[spots[1]].set(largest)


def steps_of(rng, dims, cuts, low, top_value):
    def one(axis_at, blocks):
        heights = jax.random.uniform(jax.random.fold_in(jax.random.fold_in(rng, 6), axis_at), (blocks,), jnp.float32, low / len(cuts), top_value / len(cuts))
        return jnp.repeat(jnp.exp(heights), dims[axis_at] // blocks).reshape((-1,) + (1,) * (len(dims) - axis_at - 1))

    loudness = one(*cuts[0])
    for cut in cuts[1:]:
        loudness = loudness * one(*cut)
    return loudness


def profile(count, total, limit, slope):
    portions = [(1 << 20) // math.isqrt(rank ** slope) + 1 for rank in range(2, count + 1)]
    rest, given = total - limit - (count - 1), [1] * (count - 1)
    while rest > 0:
        candidates = [i for i in range(count - 1) if given[i] < limit]
        mass, budget = sum([portions[i] for i in candidates]), rest
        for i in candidates:
            addition = min(limit - given[i], max(1, budget * portions[i] // mass), rest)
            given[i] = given[i] + addition
            rest = rest - addition
    return np.array([limit] + given)


def uneven(rng, number_of, total, most, skew):
    if number_of == 2:
        one = jax.random.randint(rng, (), max(1, total - most), min(most, total - 1) + 1)
        return jnp.stack([one, total - one])
    lengths = jnp.asarray(profile(number_of, total, most, skew), jnp.int32)
    pairs = (number_of - 1) // 2
    source_of, receiver = lengths[1:1 + 2 * pairs:2], lengths[2:2 + 2 * pairs:2]
    room = jnp.minimum(source_of - 1, most - receiver)
    shifted = jax.random.randint(jax.random.fold_in(rng, 1), (pairs,), 0, 1 << 20) % (room + 1)
    lengths = lengths.at[1:1 + 2 * pairs:2].set(source_of - shifted).at[2:2 + 2 * pairs:2].set(receiver + shifted)
    return lengths[jax.random.permutation(jax.random.fold_in(rng, 2), number_of)]


def noise(own_key, dims, spread, limit, shards=(), kind=jnp.bfloat16):
    entries = jax.random.normal(own_key, dims, jnp.float32) * spread
    if len(shards) > 0:
        entries = steps_of(own_key, dims, shards, -0.22, 0.18) * entries
    return jnp.clip(entries, min=-limit, max=limit).astype(kind)


def setup_inputs(seed: int = 0, part: int = 0) -> dict:
    splits = jax.random.split(jax.random.key(seed), 6)
    own_keys = jax.random.split(jax.random.fold_in(splits[5], part), 6)
    tokens = draw_tokens(jax.random.fold_in(jax.random.fold_in(splits[5], part), 71), part)
    blocks = noise(splits[1], (OWNERS, MAXB, BS, BS), (OWNERS * AVG * BS * BS // FFW) ** -0.5, 0.5, ((0, 16),))
    counts = jax.vmap(lambda own: uneven(own, BAL, BAL * AVG, MAXB, 2))(jax.random.split(splits[2], (OWNERS // BAL))).reshape((OWNERS // BAL, BAL)).astype(jnp.int32)
    block_rows = place_ends(jax.random.randint(splits[3], (OWNERS, MAXB), 0, ROWB), jax.random.fold_in(splits[3], 1), 0, ROWB - 1).astype(jnp.int32)
    block_cols = place_ends(jax.random.randint(splits[4], (OWNERS, MAXB), 0, COLB), jax.random.fold_in(splits[4], 1), 0, COLB - 1).astype(jnp.int32)
    return dict(tokens=tokens, blocks=blocks, counts=counts, block_rows=block_rows, block_cols=block_cols)


def reference(tokens, blocks, counts, block_rows, block_cols):
    flat = counts.reshape(-1)

    def owner_step(owner, acc):

        def slot_step(slot, inner):
            row = (block_rows[owner, slot] * BS).astype(jnp.int32)
            col = (block_cols[owner, slot] * BS).astype(jnp.int32)
            chosen = lax.dynamic_slice_in_dim(tokens, row, BS, 1)
            term = jnp.dot(chosen, blocks[owner, slot], preferred_element_type=jnp.float32)
            current = lax.dynamic_slice_in_dim(inner, col, BS, 1)
            return lax.dynamic_update_slice_in_dim(inner, current + term, col, 1)
        return lax.fori_loop(0, flat[owner], slot_step, acc)
    product = lax.fori_loop(0, OWNERS, owner_step, jnp.zeros((TOKENS, FFW), jnp.float32))
    up = product.astype(jnp.bfloat16)
    col_rms = jnp.sqrt(lax.optimization_barrier(jnp.sum(product * product, axis=0)) / TOKENS + 1e-06)
    return (up, col_rms)
```

```python
import functools

import jax
import jax.numpy as jnp
from jax import lax
from jax.experimental import pallas as pl
from jax.experimental.pallas import tpu as pltpu
from jax.sharding import PartitionSpec as P

FFW = 14336
MESH = pl.DeviceIdType.MESH
VMEM_ROOM = 67043328
VMEM_ASK = 24 * 1024 * 1024


def ring_place(chip, chips):
    odd, half = chip % 2, chip // 2
    return (1 - odd) * half + odd * (chips - 1 - half)


def chip_at(place, chips):
    high = place // (chips // 2)
    return (1 - high) * 2 * place + high * (2 * (chips - 1 - place) + 1)


def kernel(
    n, slots, ring_slots, cols,
    counts_ref, rows_ref, cols_ref, cols_v, tok_hbm, blocks_hbm, up_ref, rms_ref,
    tok_ref, blocks_ref, prev_v, last_v, prev_ref, last_ref, held, tok_s, sums, sq_s, red_s, res_s,
    ring_send, ring_recv, x_send, x_recv, pd_send, pd_recv,
    own_send, own_recv, end_send, end_recv, a_send, a_recv, b_send, b_recv, in_sem,
):
    chips = n // 2
    half = chips // 2
    edge = blocks_ref.shape[-1]
    via_x = slots - ring_slots
    me, g = lax.axis_index("blk"), lax.axis_index("groups")
    chip, core = me // 2, me % 2
    place = ring_place(chip, chips)
    partner = chip * 2 + 1 - core
    towards = [
        chip_at((place + 1) % chips, chips) * 2 + core,
        chip_at((place + chips - 1) % chips, chips) * 2 + core,
    ]

    def owner(step, way, mine=True):
        at = (place - step + chips) % chips if way == 0 else (place + step) % chips
        return chip_at(at, chips) * 2 + (core if mine else 1 - core)

    def near(i):
        return g * (slots - 1) + i * (1 - 2 * g)

    def far(i):
        return (1 - g) * (slots - 1) + i * (2 * g - 1)

    def slot_of(i):
        return near(i) if i < ring_slots else far(i - ring_slots)

    def last_list(way):
        return [i for i in range(slots) if i % 2 == way]

    blocks_in = pltpu.make_async_copy(blocks_hbm, blocks_ref, in_sem.at[0])
    tok_in = pltpu.make_async_copy(tok_hbm, tok_ref, in_sem.at[1])
    blocks_in.start()
    tok_in.start()
    barrier = pltpu.get_barrier_semaphore()
    for to in ((g, towards[0]), (g, towards[1]), (g, partner), (1 - g, me)):
        pl.semaphore_signal(barrier, inc=1, device_id=to, device_id_type=MESH)
    sums[n * slots] = jnp.zeros(sums.shape[1:], sums.dtype)
    blocks_in.wait()
    pl.semaphore_wait(barrier, 4)

    sent = []

    def ring(step, way, i, start):
        o = owner(step - 1, way) if start else owner(step, way)
        s = slot_of(i)
        src = blocks_ref.at[0, s] if start and step == 1 else held.at[o, s]
        return pltpu.make_async_remote_copy(
            src_ref=src,
            dst_ref=held.at[o, s],
            send_sem=ring_send.at[way, step - 1, i],
            recv_sem=ring_recv.at[way, step - 1, i],
            device_id=(g, towards[way]),
            device_id_type=MESH,
        )

    def cross(step, way, i, start):
        o = owner(step, way)
        s = near(i) if start else far(i)
        return pltpu.make_async_remote_copy(
            src_ref=held.at[o, s],
            dst_ref=held.at[o, s],
            send_sem=x_send.at[way, step - 1, i],
            recv_sem=x_recv.at[way, step - 1, i],
            device_id=(1 - g, me),
            device_id_type=MESH,
        )

    def pair(step, way, start):
        o = owner(step, way, start)
        return pltpu.make_async_remote_copy(
            src_ref=held.at[o],
            dst_ref=held.at[o],
            send_sem=pd_send.at[way, step - 1],
            recv_sem=pd_recv.at[way, step - 1],
            device_id=(g, partner),
            device_id_type=MESH,
        )

    def pair_end(i, start):
        o = owner(half, 0, start)
        s = slot_of(i)
        return pltpu.make_async_remote_copy(
            src_ref=held.at[o, s],
            dst_ref=held.at[o, s],
            send_sem=end_send.at[i],
            recv_sem=end_recv.at[i],
            device_id=(g, partner),
            device_id_type=MESH,
        )

    def pair_own(start):
        o = me if start else partner
        return pltpu.make_async_remote_copy(
            src_ref=blocks_ref.at[0],
            dst_ref=held.at[o],
            send_sem=own_send,
            recv_sem=own_recv,
            device_id=(g, partner),
            device_id_type=MESH,
        )

    def go(copy):
        copy.start()
        sent.append(copy)

    for i in range(ring_slots):
        for way in (0, 1):
            go(ring(1, way, i, True))
    go(pair_own(True))

    def position(o):
        apart = (ring_place(o // 2, chips) - place + chips) % chips
        step = jnp.minimum(apart, chips - apart)
        rank = jnp.where(apart < half, 2 * step, 2 * step - 1)
        rank = jnp.where(apart == half, chips - 1, rank)
        rank = jnp.where(apart == 0, 0, rank)
        return rank * 2 + jnp.where(o % 2 == core, 0, 1)

    spare = n * slots
    shape = (slots, n)
    keys = position(lax.broadcasted_iota(jnp.int32, shape, 1)) * slots
    keys = keys + lax.broadcasted_iota(jnp.int32, shape, 0)
    at_col = lax.broadcasted_iota(jnp.int32, (1, cols), 1)
    here = cols_v[...]
    prev = jnp.full(shape, -1, jnp.int32)
    last = jnp.full((1, cols), -1, jnp.int32)
    per_row = counts_ref.shape[1]
    for o in range(n):
        base = position(jnp.int32(o)) * slots
        alive = counts_ref[o // per_row, o % per_row]
        for j in range(slots):
            key = jnp.where(alive > j, base + j, -1)
            col = cols_ref[j, o]
            prev = jnp.where((here == col) & (keys > key), jnp.maximum(prev, key), prev)
            last = jnp.where(at_col == col, jnp.maximum(last, key), last)
    prev_v[...] = jnp.where(prev < 0, spare, prev)
    last_v[...] = jnp.where(last < 0, spare, last)
    tok_in.wait()
    for r in range(tok_s.shape[0]):
        tok_s[r] = tok_ref[:, r * edge : (r + 1) * edge]
    prev_in = pltpu.make_async_copy(prev_v, prev_ref, in_sem.at[2])
    last_in = pltpu.make_async_copy(last_v, last_ref, in_sem.at[3])
    prev_in.start()
    last_in.start()
    prev_in.wait()
    last_in.wait()

    def terms(o, weights, pos):
        found = []
        alive = counts_ref[o // per_row, o % per_row]
        for j in range(slots):
            found.append(
                jnp.dot(
                    tok_s[jnp.where(alive > j, rows_ref[j, o], 0)],
                    weights[j],
                    preferred_element_type=jnp.float32,
                )
            )
        for j in range(slots):
            sums[pos * slots + j] = found[j] + sums[prev_ref[j, o]]

    terms(me, blocks_ref.at[0], 0)
    pending = []

    def partner_own():
        pair_own(False).wait_recv()
        terms(partner, held.at[partner], 1)

    pending.append(partner_own)

    def ring_task(step, way, rank, mine):
        o = owner(step, way, mine)
        if not mine:
            pair(step, way, False).wait_recv()
        terms(o, held.at[o], rank * 2 + (0 if mine else 1))

    def settle(step):
        for way in (0, 1):
            for i in range(via_x):
                cross(step, way, i, False).wait_recv()
                if step + 1 == half and (ring_slots + i) in last_list(way):
                    go(ring(half, way, ring_slots + i, True))
        for way in (0, 1):
            go(pair(step, way, True))
            for mine in (True, False):
                pending.append(
                    functools.partial(ring_task, step, way, 2 * step - 1 + way, mine)
                )

    def pop():
        if pending:
            pending.pop(0)()

    for step in range(1, half):
        for i in range(ring_slots):
            for way in (0, 1):
                ring(step, way, i, False).wait_recv()
                if step + 1 < half or i in last_list(way):
                    go(ring(step + 1, way, i, True))
                if i < via_x:
                    go(cross(step, way, i, True))
            if step > 1 and i == 1:
                settle(step - 1)
            pop()
    settle(half - 1)
    pop()
    pop()
    for i in range(slots):
        ring(half, i % 2, i, False).wait_recv()
        go(pair_end(i, True))
        if i % 2 == 0 and i < slots - 1:
            pop()
    while pending:
        pop()
    ring_task(half, 0, chips - 1, True)
    for i in range(slots):
        pair_end(i, False).wait_recv()
    terms(owner(half, 0, False), held.at[owner(half, 0, False)], n - 1)

    share = cols // n
    scatter, spread, up_out = {}, [], []
    wide = share * edge
    order = sorted(range(1, n), key=lambda e: abs(e - n // 2)) + [0]
    for at, e in enumerate(order):
        o = (me + e) % n
        found = []
        for j in range(share):
            c = o * share + j
            value = sums[last_ref[0, c]]
            up_ref[:, pl.ds(pl.multiple_of(c * edge, edge), edge)] = value.astype(up_ref.dtype)
            found.append(jnp.sum(value * value, axis=0, keepdims=True))
        sq_s[o] = jnp.concatenate(found, axis=0)
        if at > 0:
            before = order[at - 1]
            to = (me + before) % n
            scatter[before] = pltpu.make_async_remote_copy(
                src_ref=sq_s.at[to],
                dst_ref=red_s.at[before],
                send_sem=a_send.at[before],
                recv_sem=a_recv.at[before],
                device_id=(g, to),
                device_id_type=MESH,
            )
            scatter[before].start()
    total = sq_s[me]
    for e in range(1, n):
        scatter[e].wait_recv()
        total = total + red_s[e]
    res_s[me] = jnp.sqrt(total / (tok_ref.shape[0] * n) + 1e-06)
    for e in range(1, n):
        to = (me + e) % n
        spread.append(
            pltpu.make_async_remote_copy(
                src_ref=res_s.at[me],
                dst_ref=res_s.at[me],
                send_sem=b_send.at[e],
                recv_sem=b_recv.at[e],
                device_id=(g, to),
                device_id_type=MESH,
            )
        )
        spread[-1].start()
    for copy in sent + list(scatter.values()):
        copy.wait_send()
    for e in range(1, n):
        origin = (me + n - e) % n
        pltpu.make_async_remote_copy(
            src_ref=res_s.at[origin],
            dst_ref=res_s.at[origin],
            send_sem=b_send.at[e],
            recv_sem=b_recv.at[e],
            device_id=(g, origin),
            device_id_type=MESH,
        ).wait_recv()
    for copy in spread:
        copy.wait_send()
    for o in range(n):
        rms_ref[o * share : (o + 1) * share, :] = res_s[o]


def per_device(n, tokens, blocks, counts, block_rows, block_cols):
    toks, width = tokens.shape
    _, slots, edge, _ = blocks.shape
    cols = FFW // edge
    share = cols // n
    half = n // 4
    ring_slots = slots - slots * 2 // 7
    via_x = slots - ring_slots
    rows, places = block_rows.T, block_cols.T
    hbm = pl.BlockSpec(memory_space=pltpu.HBM)
    vmem = pl.BlockSpec(memory_space=pltpu.VMEM)
    smem = pl.BlockSpec(memory_space=pltpu.SMEM)
    dma = pltpu.SemaphoreType.DMA
    up, rms = pl.pallas_call(
        functools.partial(kernel, n, slots, ring_slots, cols),
        out_shape=(
            jax.ShapeDtypeStruct((toks, FFW), jnp.bfloat16),
            jax.ShapeDtypeStruct((cols, edge), jnp.float32),
        ),
        in_specs=[smem, smem, smem, vmem, hbm, hbm],
        out_specs=(vmem, vmem),
        scratch_shapes=[
            pltpu.VMEM(tokens.shape, jnp.bfloat16),
            pltpu.VMEM(blocks.shape, jnp.bfloat16),
            pltpu.VMEM(places.shape, jnp.int32),
            pltpu.VMEM((1, cols), jnp.int32),
            pltpu.SMEM(places.shape, jnp.int32),
            pltpu.SMEM((1, cols), jnp.int32),
            pltpu.VMEM((n, slots, edge, edge), jnp.bfloat16),
            pltpu.VMEM((width // edge, toks, edge), jnp.bfloat16),
            pltpu.VMEM((n * slots + 1, toks, edge), jnp.float32),
            pltpu.VMEM((n, share, edge), jnp.float32),
            pltpu.VMEM((n, share, edge), jnp.float32),
            pltpu.VMEM((n, share, edge), jnp.float32),
            dma((2, half, slots)),
            dma((2, half, slots)),
            dma((2, half, via_x)),
            dma((2, half, via_x)),
            dma((2, half)),
            dma((2, half)),
            dma,
            dma,
            dma((slots,)),
            dma((slots,)),
            dma((n,)),
            dma((n,)),
            dma((n,)),
            dma((n,)),
            dma((4,)),
        ],
        compiler_params=pltpu.CompilerParams(
            collective_id=0, has_side_effects=True, vmem_limit_bytes=VMEM_ASK
        ),
    )(*[pltpu.with_memory_space_constraint(v, pltpu.HBM) for v in (counts, rows, places, places, tokens, blocks)])
    return up, rms.reshape(-1)


def make_fold(token_grid, rows_table, cols_table, live_table, col_blocks):
    row_blocks = token_grid.shape[1]

    def fold(carry, piece, start):
        rows = rows_table.reshape(-1)
        cols = cols_table.reshape(-1)
        live = live_table.reshape(-1)
        weights = piece.reshape(-1, piece.shape[2], piece.shape[3])
        weights = jnp.where(live[:, None, None], weights, jnp.zeros_like(weights))
        row_pick = (rows[:, None] == jnp.arange(row_blocks, dtype=jnp.int32)[None, :]).astype(
            jnp.bfloat16
        )
        chosen = jnp.einsum(
            "trk,br->tbk", token_grid, row_pick, preferred_element_type=jnp.float32
        ).astype(jnp.bfloat16)
        terms = jnp.einsum("tbk,bkn->tbn", chosen, weights, preferred_element_type=jnp.float32)
        col_pick = (cols[:, None] == jnp.arange(col_blocks, dtype=jnp.int32)[None, :]).astype(
            jnp.float32
        )
        placed = jnp.einsum(
            "tbn,bc->tcn",
            terms,
            col_pick,
            precision=lax.Precision.HIGHEST,
            preferred_element_type=jnp.float32,
        )
        return placed.reshape(carry.shape)

    return fold


def by_collectives(tokens, blocks, counts, block_rows, block_cols):
    tok_count = tokens.shape[0]
    edge = blocks.shape[2]
    slots = blocks.shape[1]
    token_grid = tokens.reshape(tok_count, -1, edge)
    col_blocks = FFW // edge
    empty = jnp.zeros((tok_count, FFW), jnp.float32)
    live_table = counts.reshape(-1)[:, None] > jnp.arange(slots, dtype=jnp.int32)[None, :]
    fold = make_fold(token_grid, block_rows, block_cols, live_table, col_blocks)
    product = fold(empty, lax.all_gather(blocks, "blk", axis=0, tiled=True), jnp.int32(0))
    up = product.astype(jnp.bfloat16)
    squares = lax.psum(jnp.sum(product * product, axis=0), "blk")
    col_rms = jnp.sqrt(squares / (tok_count * lax.axis_size("blk")) + 1e-06)
    return (up, col_rms)


def solution(mesh):
    n, groups = mesh.shape["blk"], mesh.shape["groups"]

    def body(tokens, blocks, counts, block_rows, block_cols):
        owned, slots, edge, _ = blocks.shape
        cols = FFW // edge
        need = n * slots * edge * (2 * edge + 4 * tokens.shape[0])
        fits = need + 2 * tokens.shape[0] * (FFW + tokens.shape[1]) < VMEM_ROOM // 2
        if groups == 2 and owned == 1 and n % 4 == 0 and n >= 8 and cols % n == 0 and fits:
            return per_device(n, tokens, blocks, counts, block_rows, block_cols)
        return by_collectives(tokens, blocks, counts, block_rows, block_cols)

    placed = (P(("groups", "blk"), None), P("blk", None, None, None), P(), P(), P())
    return jax.shard_map(
        body,
        mesh=mesh,
        in_specs=placed,
        out_specs=(P(("groups", "blk"), None), P("groups")),
        check_vma=False,
    )
```
